32 devices in a mesh: lat: 4 (over x, core), lon: 4 (over z), lev: 2 (over y).
Axes of the slice: x: 2, y: 2, z: 4, core: 2. Of those that a mesh axis runs over, the one named last changes fastest.
Arguments:
- initial_heat: float32 [128, 512, 8, 128], P('lat', 'lon', 'lev'), may hold values from 0.5 to 2
- diffusivity_ratio: float32 [128, 512, 8, 128], P('lat', 'lon', 'lev'), may hold values from 0.03 to 0.15
- forcing_term: float32 [128, 512, 8, 128], P('lat', 'lon', 'lev'), may hold values from -0.2 to 0.2
Outputs:
- standard_deviation_score: float32 [128, 512, 8, 128], P('lat', 'lon', 'lev')
- temperature_end: float32 [128, 512, 8, 128], P('lat', 'lon', 'lev')
The draws below stay inside these ranges and needn't reach their ends.
All inputs are finite; a program needn't handle non-finite values.
Results may differ from the reference program's by a relative error of at most 0.00002.
Values sent between devices are 32-bit elements; how exact they have to be, the bound alone decides.
A program may use at most 128 MiB of HBM per device.

```python
import jax
import jax.numpy as jnp
from jax import lax

GRID_DEPTH = 128
GRID_WIDTH = 512
GRID_HEIGHT = 8
MEMBER_TOTAL = 128
STEPS = 4


def steps_of(key, shape, cuts, least, top_value):
    level = 1.0
    for dim, shards_of in cuts:
        draws = jax.random.uniform(jax.random.fold_in(jax.random.fold_in(key, 6), dim), (shards_of,), jnp.float32, least / len(cuts), top_value / len(cuts))
        level = level * jnp.repeat(jnp.exp(draws), shape[dim] // shards_of).reshape((-1,) + (1,) * (len(shape) - 1 - dim))
    return level


def setup_inputs(seed: int = 0) -> dict:
    key_of = jax.random.split(jax.random.key(seed), 4)
    return {
        "initial_heat": jnp.clip(0.5 + 1.5 * jax.random.uniform(key_of[0], (GRID_DEPTH, GRID_WIDTH, GRID_HEIGHT, MEMBER_TOTAL), jnp.float32) ** steps_of(key_of[0], (GRID_DEPTH, GRID_WIDTH, GRID_HEIGHT, MEMBER_TOTAL), ((0, 4), (1, 4), (2, 2)), -0.2, 0.2), 0.5, 2.0),
        "diffusivity_ratio": jnp.clip(0.03 + 0.120000007 * jax.random.uniform(key_of[1], (GRID_DEPTH, GRID_WIDTH, GRID_HEIGHT, MEMBER_TOTAL), jnp.float32) ** steps_of(key_of[1], (GRID_DEPTH, GRID_WIDTH, GRID_HEIGHT, MEMBER_TOTAL), ((0, 4), (1, 4), (2, 2)), -0.2, 0.2), 0.03, 0.15),
        "forcing_term": jnp.clip(jax.random.uniform(key_of[2], (GRID_DEPTH, GRID_WIDTH, GRID_HEIGHT, MEMBER_TOTAL), jnp.float32, -0.2, 0.2) * steps_of(key_of[2], (GRID_DEPTH, GRID_WIDTH, GRID_HEIGHT, MEMBER_TOTAL), ((0, 4), (1, 4), (2, 2)), -0.4, 0.0), -0.2, 0.2),
    }


def without_rim(values, dims):
    for dim in dims:
        values = lax.slice_in_dim(values, 1, values.shape[dim] - 1, axis=dim)
    return values

def shifted_cells(values, dim, start, dims):
    others = [other for other in dims if other != dim]
    values = without_rim(values, others)
    return lax.slice_in_dim(values, start, start + values.shape[dim] - 2, axis=dim)

def march_forward(extended_grid_state, diffusivity_ratio, forcing_term):
    middle = without_rim(extended_grid_state, (0, 1, 2))
    lower = [shifted_cells(extended_grid_state, dim, 0, (0, 1, 2)) for dim in (0, 1, 2)]
    upper = [shifted_cells(extended_grid_state, dim, 2, (0, 1, 2)) for dim in (0, 1, 2)]
    spread = lower[0] + upper[0] + lower[1] + upper[1] + lower[2] + upper[2] - 6.0 * middle
    return middle + diffusivity_ratio * spread + forcing_term

def reference(initial_heat, diffusivity_ratio, forcing_term):
    for step in range(STEPS):
        initial_heat = march_forward(jnp.pad(initial_heat, ((1, 1), (1, 1), (1, 1), (0, 0)), mode='wrap'), diffusivity_ratio, forcing_term)
    row_mean_estimate = lax.optimization_barrier(jnp.mean(initial_heat, axis=1, keepdims=True))
    deviations_from_mean = initial_heat - row_mean_estimate
    line_variance = lax.optimization_barrier(jnp.mean(deviations_from_mean * deviations_from_mean, axis=1, keepdims=True))
    standard_deviation_score = deviations_from_mean * lax.rsqrt(line_variance + 0.0001)
    return (standard_deviation_score, initial_heat)
```

```python
import functools

import jax
import jax.numpy as jnp
from jax import lax
from jax.experimental import pallas as pl
from jax.experimental.pallas import tpu as pltpu
from jax.sharding import PartitionSpec as P

STEPS = 4
PAD = 8
XBLOCK = 32
MESH = pl.DeviceIdType.MESH


def march_kernel(
    sizes, chunks, rows,
    heat_in, ratio_in, forcing_in, heat_out, moments_out,
    field, raw, ratio, forcing, xsend, xrecv, stats,
    load_heat, load_ratio, load_forcing, store_heat,
    zsend_sem, zrecv_sem, xsend_sem, xrecv_sem, ysend_sem, yrecv_sem, stat_send, stat_recv,
):
    depth, width, height = sizes
    inner = pl.ds(PAD, width)
    places = {axis: lax.axis_index(axis) for axis in ("lat", "lon", "lev")}
    counts = {axis: lax.axis_size(axis) for axis in ("lat", "lon", "lev")}

    def beside(axis, offset):
        return {axis: lax.rem(places[axis] + offset + counts[axis], counts[axis])}

    def rows_of(c):
        return pl.ds(c * rows, rows)

    def load(c):
        return [
            pltpu.make_async_copy(source.at[rows_of(c)], target.at[rows_of(c)], sem.at[c])
            for source, target, sem in (
                (heat_in, raw, load_heat), (ratio_in, ratio, load_ratio), (forcing_in, forcing, load_forcing),
            )
        ]

    def out_copy(c):
        return pltpu.make_async_copy(raw.at[rows_of(c)], heat_out.at[rows_of(c)], store_heat.at[c])

    def zcopy(side, p, c):
        span = pl.ds(1 + c * rows, rows)
        return pltpu.make_async_remote_copy(
            src_ref=field.at[p, (1, height)[side], span, inner],
            dst_ref=field.at[p, (height + 1, 0)[side], span, inner],
            send_sem=zsend_sem.at[side, p, c], recv_sem=zrecv_sem.at[1 - side, p, c],
            device_id=beside("lev", (-1, 1)[side]), device_id_type=MESH,
        )

    def xcopy(side, p, c):
        return pltpu.make_async_remote_copy(
            src_ref=xsend.at[side, p, c], dst_ref=xrecv.at[1 - side, p, c],
            send_sem=xsend_sem.at[side, p, c], recv_sem=xrecv_sem.at[1 - side, p, c],
            device_id=beside("lon", (-1, 1)[side]), device_id_type=MESH,
        )

    def ycopy(side, p):
        return pltpu.make_async_remote_copy(
            src_ref=field.at[p, pl.ds(1, height), (1, depth)[side], inner],
            dst_ref=field.at[p, pl.ds(1, height), (depth + 1, 0)[side], inner],
            send_sem=ysend_sem.at[side, p], recv_sem=yrecv_sem.at[1 - side, p],
            device_id=beside("lat", (-1, 1)[side]), device_id_type=MESH,
        )

    def stat_copy(offset, c):
        return pltpu.make_async_remote_copy(
            src_ref=stats.at[0, c], dst_ref=stats.at[offset, c],
            send_sem=stat_send.at[offset - 1, c], recv_sem=stat_recv.at[offset - 1, c],
            device_id=beside("lon", offset), device_id_type=MESH,
        )

    def send(p, c):
        for side, end in ((0, 0), (1, chunks - 1)):
            @pl.when(c == end)
            def _():
                ycopy(side, p).start()
        for side in (0, 1):
            zcopy(side, p, c).start()
        for side in (0, 1):
            xcopy(side, p, c).start()

    def sent(p, c):
        for side, end in ((0, 0), (1, chunks - 1)):
            @pl.when(c == end)
            def _():
                ycopy(side, p).wait_send()
        for side in (0, 1):
            zcopy(side, p, c).wait_send()
            xcopy(side, p, c).wait_send()

    def arrived(p, c):
        for side, end in ((1, 0), (0, chunks - 1)):
            @pl.when(c == end)
            def _():
                ycopy(side, p).wait_recv()
        for side in (0, 1):
            xcopy(side, p, c).wait_recv()
        for side in (0, 1):
            zcopy(side, p, c).wait_recv()

    def pack(p, c, i):
        for z in range(height):
            for side, x in ((0, PAD), (1, PAD + width - 1)):
                xsend[side, p, c, pl.ds(i * height + z, 1), :] = field[p, z + 1, c * rows + i + 1, pl.ds(x, 1), :]

    def start_loads(c, carry):
        load(c)[0].start()
        return carry

    def start_others(c, carry):
        for copy in load(c)[1:]:
            copy.start()
        return carry

    lax.fori_loop(0, chunks, start_loads, 0)
    lax.fori_loop(0, chunks, start_others, 0)

    barrier = pltpu.get_barrier_semaphore()
    greeted = [beside("lev", -1), beside("lev", 1), beside("lat", -1), beside("lat", 1)]
    greeted += [beside("lon", offset) for offset in range(1, counts["lon"])]
    for device in greeted:
        pl.semaphore_signal(barrier, inc=1, device_id=device, device_id_type=MESH)
    pl.semaphore_wait(barrier, len(greeted))

    def unpack(c, carry):
        load(c)[0].wait()

        def row(i, carry):
            y = c * rows + i
            for z in range(height):
                field[0, z + 1, y + 1, inner, :] = raw[y, pl.ds(z, width, stride=height), :]
            pack(0, c, i)
            return carry

        lax.fori_loop(0, rows, row, 0)
        send(0, c)
        return carry

    lax.fori_loop(0, chunks, unpack, 0)

    def step(s, carry):
        p = lax.rem(s, 2)
        q = 1 - p

        def chunk(c, carry):
            @pl.when(s == 0)
            def _():
                for copy in load(c)[1:]:
                    copy.wait()

            @pl.when(s >= 1)
            def _():
                sent(q, c)

            arrived(p, c)

            def row(i, carry):
                y = c * rows + i
                for z in range(height):
                    for side, x in ((0, PAD - 1), (1, PAD + width)):
                        field[p, z + 1, y + 1, pl.ds(x, 1), :] = xrecv[side, p, c, pl.ds(i * height + z, 1), :]
                for x in range(0, width, XBLOCK):
                    here = pl.ds(PAD + x, XBLOCK)
                    planes = [field[p, z, y + 1, here, :] for z in range(height + 2)]
                    for z in range(height):
                        middle = planes[z + 1]
                        spread = (
                            field[p, z + 1, y, here, :] + field[p, z + 1, y + 2, here, :]
                            + field[p, z + 1, y + 1, pl.ds(PAD + x - 1, XBLOCK), :]
                            + field[p, z + 1, y + 1, pl.ds(PAD + x + 1, XBLOCK), :]
                            + planes[z] + planes[z + 2] - 6.0 * middle
                        )
                        cells = pl.ds(x * height + z, XBLOCK, stride=height)
                        field[q, z + 1, y + 1, here, :] = middle + ratio[y, cells, :] * spread + forcing[y, cells, :]
                pack(q, c, i)
                return carry

            lax.fori_loop(0, rows, row, 0)

            @pl.when(s < STEPS - 1)
            def _():
                send(q, c)

            @pl.when(s == STEPS - 1)
            def _():
                def finish(i, carry):
                    y = c * rows + i
                    for z in range(height):
                        line = field[q, z + 1, y + 1, inner, :]
                        raw[y, pl.ds(z, width, stride=height), :] = line
                        mean = jnp.sum(line, axis=0, keepdims=True) * (1.0 / width)
                        centred = line - mean
                        stats[0, c, 0, pl.ds(i * height + z, 1), :] = mean
                        stats[0, c, 1, pl.ds(i * height + z, 1), :] = jnp.sum(centred * centred, axis=0, keepdims=True)
                    return carry

                lax.fori_loop(0, rows, finish, 0)
                for offset in range(1, counts["lon"]):
                    stat_copy(offset, c).start()
                out_copy(c).start()

            return carry

        lax.fori_loop(0, chunks, chunk, 0)
        return carry

    lax.fori_loop(0, STEPS, step, 0)

    def combine(c, carry):
        for offset in range(1, counts["lon"]):
            stat_copy(offset, c).wait_recv()
        means = [stats[offset, c, 0] for offset in range(counts["lon"])]
        mean = sum(means[1:], means[0]) * (1.0 / counts["lon"])
        squares = sum([stats[offset, c, 1] for offset in range(1, counts["lon"])], stats[0, c, 1])
        apart = sum([(other - mean) * (other - mean) for other in means[1:]], (means[0] - mean) * (means[0] - mean))
        variance = (squares + width * apart) * (1.0 / (width * counts["lon"]))
        scale = lax.rsqrt(variance + 0.0001)
        for i in range(rows):
            for half in range(2):
                for kind, values in ((0, mean), (1, scale)):
                    moments_out[kind, c * rows + i, pl.ds(half * height, height), :] = values[i * height:(i + 1) * height]
        return carry

    lax.fori_loop(0, chunks, combine, 0)

    def drain(c, carry):
        sent((STEPS - 1) % 2, c)
        for offset in range(1, counts["lon"]):
            stat_copy(offset, c).wait_send()
        out_copy(c).wait()
        return carry

    lax.fori_loop(0, chunks, drain, 0)


def score_kernel(heat, moments, score, end):
    for i in range(heat.shape[0]):
        mean, scale = moments[0, i], moments[1, i]
        values = heat[i]
        end[i] = values
        tall = values.reshape(values.shape[0] // mean.shape[0], *mean.shape)
        score[i] = ((tall - mean[None]) * scale[None]).reshape(values.shape)


def local(initial_heat, diffusivity_ratio, forcing_term):
    depth, width, height, members = initial_heat.shape
    rows = 4
    chunks = depth // rows
    lon = lax.axis_size("lon")
    flat = (depth, width * height, members)
    f32 = jnp.float32
    anywhere = pl.BlockSpec(memory_space=pl.ANY)
    dma = pltpu.SemaphoreType.DMA
    heat, moments = pl.pallas_call(
        functools.partial(march_kernel, (depth, width, height), chunks, rows),
        out_shape=(jax.ShapeDtypeStruct(flat, f32), jax.ShapeDtypeStruct((2, depth, 2 * height, members), f32)),
        in_specs=[anywhere] * 3,
        out_specs=(anywhere, pl.BlockSpec(memory_space=pltpu.VMEM)),
        scratch_shapes=[
            pltpu.VMEM((2, height + 2, depth + 2, width + 2 * PAD, members), f32),
            pltpu.VMEM(flat, f32),
            pltpu.VMEM(flat, f32),
            pltpu.VMEM(flat, f32),
            pltpu.VMEM((2, 2, chunks, rows * height, members), f32),
            pltpu.VMEM((2, 2, chunks, rows * height, members), f32),
            pltpu.VMEM((lon, chunks, 2, rows * height, members), f32),
            dma((chunks,)), dma((chunks,)), dma((chunks,)), dma((chunks,)),
            dma((2, 2, chunks)), dma((2, 2, chunks)),
            dma((2, 2, chunks)), dma((2, 2, chunks)),
            dma((2, 2)), dma((2, 2)),
            dma((lon - 1, chunks)), dma((lon - 1, chunks)),
        ],
        compiler_params=pltpu.CompilerParams(
            collective_id=0, has_side_effects=True, vmem_limit_bytes=60 * 1024 * 1024
        ),
        name="march",
    )(*[a.reshape(flat) for a in (initial_heat, diffusivity_ratio, forcing_term)])
    part = 4
    block = pl.BlockSpec((part,) + flat[1:], lambda i: (i, 0, 0))
    score, end = pl.pallas_call(
        score_kernel,
        grid=(depth // part,),
        out_shape=(jax.ShapeDtypeStruct(flat, f32),) * 2,
        in_specs=[block, pl.BlockSpec((2, part, 2 * height, members), lambda i: (0, i, 0, 0))],
        out_specs=(block, block),
        name="score",
    )(heat, moments)
    return score.reshape(initial_heat.shape), end.reshape(initial_heat.shape)


def solution(mesh):
    placed = P("lat", "lon", "lev", None)
    return jax.shard_map(
        local, mesh=mesh, in_specs=(placed,) * 3, out_specs=(placed,) * 2, check_vma=False
    )
```

```python
import functools

import jax
import jax.numpy as jnp
from jax import lax
from jax.experimental import pallas as pl
from jax.experimental.pallas import tpu as pltpu
from jax.sharding import PartitionSpec as P

STEPS = 4
PAD = 8
XBLOCK = 32
MESH = pl.DeviceIdType.MESH


def march_kernel(
    sizes, chunks, rows,
    heat_in, ratio_in, forcing_in, raw, moments_out,
    field, ratio, forcing, xsend, xrecv, stats,
    load_heat, load_ratio, load_forcing,
    zsend_sem, zrecv_sem, xsend_sem, xrecv_sem, ysend_sem, yrecv_sem, stat_send, stat_recv,
):
    depth, width, height = sizes
    inner = pl.ds(PAD, width)
    places = {axis: lax.axis_index(axis) for axis in ("lat", "lon", "lev")}
    counts = {axis: lax.axis_size(axis) for axis in ("lat", "lon", "lev")}

    def beside(axis, offset):
        return {axis: lax.rem(places[axis] + offset + counts[axis], counts[axis])}

    def rows_of(c):
        return pl.ds(c * rows, rows)

    def load(c):
        return [
            pltpu.make_async_copy(source.at[rows_of(c)], target.at[rows_of(c)], sem.at[c])
            for source, target, sem in (
                (heat_in, raw, load_heat), (ratio_in, ratio, load_ratio), (forcing_in, forcing, load_forcing),
            )
        ]

    def zcopy(side, p, c):
        span = pl.ds(1 + c * rows, rows)
        return pltpu.make_async_remote_copy(
            src_ref=field.at[p, (1, height)[side], span, inner],
            dst_ref=field.at[p, (height + 1, 0)[side], span, inner],
            send_sem=zsend_sem.at[side, p, c], recv_sem=zrecv_sem.at[1 - side, p, c],
            device_id=beside("lev", (-1, 1)[side]), device_id_type=MESH,
        )

    def xcopy(side, p, c):
        return pltpu.make_async_remote_copy(
            src_ref=xsend.at[side, p, c], dst_ref=xrecv.at[1 - side, p, c],
            send_sem=xsend_sem.at[side, p, c], recv_sem=xrecv_sem.at[1 - side, p, c],
            device_id=beside("lon", (-1, 1)[side]), device_id_type=MESH,
        )

    def ycopy(side, p):
        return pltpu.make_async_remote_copy(
            src_ref=field.at[p, pl.ds(1, height), (1, depth)[side], inner],
            dst_ref=field.at[p, pl.ds(1, height), (depth + 1, 0)[side], inner],
            send_sem=ysend_sem.at[side, p], recv_sem=yrecv_sem.at[1 - side, p],
            device_id=beside("lat", (-1, 1)[side]), device_id_type=MESH,
        )

    def stat_copy(offset, c):
        return pltpu.make_async_remote_copy(
            src_ref=stats.at[0, c], dst_ref=stats.at[offset, c],
            send_sem=stat_send.at[offset - 1, c], recv_sem=stat_recv.at[offset - 1, c],
            device_id=beside("lon", offset), device_id_type=MESH,
        )

    def send(p, c):
        for side, end in ((0, 0), (1, chunks - 1)):
            @pl.when(c == end)
            def _():
                ycopy(side, p).start()
        for side in (0, 1):
            zcopy(side, p, c).start()
        for side in (0, 1):
            xcopy(side, p, c).start()

    def sent(p, c):
        for side, end in ((0, 0), (1, chunks - 1)):
            @pl.when(c == end)
            def _():
                ycopy(side, p).wait_send()
        for side in (0, 1):
            zcopy(side, p, c).wait_send()
            xcopy(side, p, c).wait_send()

    def arrived(p, c):
        for side, end in ((1, 0), (0, chunks - 1)):
            @pl.when(c == end)
            def _():
                ycopy(side, p).wait_recv()
        for side in (0, 1):
            xcopy(side, p, c).wait_recv()
        for side in (0, 1):
            zcopy(side, p, c).wait_recv()

    def pack(p, c, i):
        for z in range(height):
            for side, x in ((0, PAD), (1, PAD + width - 1)):
                xsend[side, p, c, pl.ds(i * height + z, 1), :] = field[p, z + 1, c * rows + i + 1, pl.ds(x, 1), :]

    def start_loads(c, carry):
        load(c)[0].start()
        return carry

    def start_others(c, carry):
        for copy in load(c)[1:]:
            copy.start()
        return carry

    lax.fori_loop(0, chunks, start_loads, 0)
    lax.fori_loop(0, chunks, start_others, 0)

    barrier = pltpu.get_barrier_semaphore()
    greeted = [beside("lev", -1), beside("lev", 1), beside("lat", -1), beside("lat", 1)]
    greeted += [beside("lon", offset) for offset in range(1, counts["lon"])]
    for device in greeted:
        pl.semaphore_signal(barrier, inc=1, device_id=device, device_id_type=MESH)

    def unpack(c):
        load(c)[0].wait()

        def row(i, carry):
            y = c * rows + i
            for z in range(height):
                field[0, z + 1, y + 1, inner, :] = raw[y, pl.ds(z, width, stride=height), :]
            pack(0, c, i)
            return carry

        lax.fori_loop(0, rows, row, 0)

    def unpack_send(c, carry):
        unpack(c)
        send(0, c)
        return carry

    unpack(0)
    pl.semaphore_wait(barrier, len(greeted))
    send(0, 0)
    lax.fori_loop(1, chunks, unpack_send, 0)

    def combine(c):
        for offset in range(1, counts["lon"]):
            stat_copy(offset, c).wait_recv()
        means = [stats[offset, c, 0] for offset in range(counts["lon"])]
        mean = sum(means[1:], means[0]) * (1.0 / counts["lon"])
        squares = sum([stats[offset, c, 1] for offset in range(1, counts["lon"])], stats[0, c, 1])
        apart = sum([(other - mean) * (other - mean) for other in means[1:]], (means[0] - mean) * (means[0] - mean))
        variance = (squares + width * apart) * (1.0 / (width * counts["lon"]))
        scale = lax.rsqrt(variance + 0.0001)
        for i in range(rows):
            for half in range(2):
                for kind, values in ((0, mean), (1, scale)):
                    moments_out[kind, c * rows + i, pl.ds(half * height, height), :] = values[i * height:(i + 1) * height]
        for offset in range(1, counts["lon"]):
            stat_copy(offset, c).wait_send()
        sent((STEPS - 1) % 2, c)

    def step(s, carry):
        p = lax.rem(s, 2)
        q = 1 - p

        def chunk(c, carry):
            @pl.when(s == 0)
            def _():
                for copy in load(c)[1:]:
                    copy.wait()

            @pl.when(s >= 1)
            def _():
                sent(q, c)

            arrived(p, c)

            def row(i, carry):
                y = c * rows + i
                for z in range(height):
                    for side, x in ((0, PAD - 1), (1, PAD + width)):
                        field[p, z + 1, y + 1, pl.ds(x, 1), :] = xrecv[side, p, c, pl.ds(i * height + z, 1), :]
                for x in range(0, width, XBLOCK):
                    here = pl.ds(PAD + x, XBLOCK)
                    planes = [field[p, z, y + 1, here, :] for z in range(height + 2)]
                    for z in range(height):
                        middle = planes[z + 1]
                        spread = (
                            field[p, z + 1, y, here, :] + field[p, z + 1, y + 2, here, :]
                            + field[p, z + 1, y + 1, pl.ds(PAD + x - 1, XBLOCK), :]
                            + field[p, z + 1, y + 1, pl.ds(PAD + x + 1, XBLOCK), :]
                            + planes[z] + planes[z + 2] - 6.0 * middle
                        )
                        cells = pl.ds(x * height + z, XBLOCK, stride=height)
                        field[q, z + 1, y + 1, here, :] = middle + ratio[y, cells, :] * spread + forcing[y, cells, :]
                pack(q, c, i)
                return carry

            lax.fori_loop(0, rows, row, 0)

            @pl.when(s < STEPS - 1)
            def _():
                send(q, c)

            @pl.when(s == STEPS - 1)
            def _():
                def finish(i, carry):
                    y = c * rows + i
                    for z in range(height):
                        line = field[q, z + 1, y + 1, inner, :]
                        raw[y, pl.ds(z, width, stride=height), :] = line
                        mean = jnp.sum(line, axis=0, keepdims=True) * (1.0 / width)
                        centred = line - mean
                        stats[0, c, 0, pl.ds(i * height + z, 1), :] = mean
                        stats[0, c, 1, pl.ds(i * height + z, 1), :] = jnp.sum(centred * centred, axis=0, keepdims=True)
                    return carry

                lax.fori_loop(0, rows, finish, 0)
                for offset in range(1, counts["lon"]):
                    stat_copy(offset, c).start()

                @pl.when(c >= 1)
                def _():
                    combine(c - 1)

            return carry

        lax.fori_loop(0, chunks, chunk, 0)
        return carry

    lax.fori_loop(0, STEPS, step, 0)


    combine(chunks - 1)


def score_kernel(chunks, heat, moments, score, end, scaled, score_sem, end_sem):
    rows = heat.shape[0] // chunks
    finish = pltpu.make_async_copy(heat, end, end_sem)
    finish.start()

    def out_copy(c):
        span = pl.ds(c * rows, rows)
        return pltpu.make_async_copy(scaled.at[span], score.at[span], score_sem.at[c])

    def chunk(c, carry):
        def row(i, carry):
            y = c * rows + i
            mean, scale = moments[0, y], moments[1, y]
            values = heat[y]
            tall = values.reshape(values.shape[0] // mean.shape[0], *mean.shape)
            scaled[y] = ((tall - mean[None]) * scale[None]).reshape(values.shape)
            return carry

        lax.fori_loop(0, rows, row, 0)
        out_copy(c).start()
        return carry

    def drain(c, carry):
        out_copy(c).wait()
        return carry

    lax.fori_loop(0, chunks, chunk, 0)
    lax.fori_loop(0, chunks, drain, 0)
    finish.wait()


def local(initial_heat, diffusivity_ratio, forcing_term):
    depth, width, height, members = initial_heat.shape
    rows = 2
    chunks = depth // rows
    lon = lax.axis_size("lon")
    flat = (depth, width * height, members)
    f32 = jnp.float32
    anywhere = pl.BlockSpec(memory_space=pl.ANY)
    dma = pltpu.SemaphoreType.DMA
    heat, moments = pl.pallas_call(
        functools.partial(march_kernel, (depth, width, height), chunks, rows),
        out_shape=(pltpu.VMEM(flat, f32), pltpu.VMEM((2, depth, 2 * height, members), f32)),
        in_specs=[anywhere] * 3,
        out_specs=(pl.BlockSpec(memory_space=pltpu.VMEM),) * 2,
        scratch_shapes=[
            pltpu.VMEM((2, height + 2, depth + 2, width + 2 * PAD, members), f32),
            pltpu.VMEM(flat, f32),
            pltpu.VMEM(flat, f32),
            pltpu.VMEM((2, 2, chunks, rows * height, members), f32),
            pltpu.VMEM((2, 2, chunks, rows * height, members), f32),
            pltpu.VMEM((lon, chunks, 2, rows * height, members), f32),
            dma((chunks,)), dma((chunks,)), dma((chunks,)),
            dma((2, 2, chunks)), dma((2, 2, chunks)),
            dma((2, 2, chunks)), dma((2, 2, chunks)),
            dma((2, 2)), dma((2, 2)),
            dma((lon - 1, chunks)), dma((lon - 1, chunks)),
        ],
        compiler_params=pltpu.CompilerParams(
            collective_id=0, has_side_effects=True, vmem_limit_bytes=48 * 1024 * 1024
        ),
        name="march",
    )(*[a.reshape(flat) for a in (initial_heat, diffusivity_ratio, forcing_term)])
    parts = min(8, depth)
    score, end = pl.pallas_call(
        functools.partial(score_kernel, parts),
        out_shape=(jax.ShapeDtypeStruct(flat, f32),) * 2,
        in_specs=[pl.BlockSpec(memory_space=pltpu.VMEM)] * 2,
        out_specs=(anywhere,) * 2,
        scratch_shapes=[pltpu.VMEM(flat, f32), dma((parts,)), dma(())],
        compiler_params=pltpu.CompilerParams(vmem_limit_bytes=24 * 1024 * 1024),
        name="score",
    )(heat, moments)
    return score.reshape(initial_heat.shape), end.reshape(initial_heat.shape)


def solution(mesh):
    placed = P("lat", "lon", "lev", None)
    return jax.shard_map(
        local, mesh=mesh, in_specs=(placed,) * 3, out_specs=(placed,) * 2, check_vma=False
    )
```

```python
import functools

import jax
import jax.numpy as jnp
from jax import lax
from jax.experimental import pallas as pl
from jax.experimental.pallas import tpu as pltpu
from jax.sharding import PartitionSpec as P

STEPS = 4
PAD = 8
XBLOCK = 32
MESH = pl.DeviceIdType.MESH


def march_kernel(
    sizes, chunks, rows,
    heat_in, ratio_in, forcing_in, raw, moments_out,
    field, ratio, forcing, xsend, xrecv, stats,
    load_heat, load_ratio, load_forcing,
    zsend_sem, zrecv_sem, xsend_sem, xrecv_sem, ysend_sem, yrecv_sem, stat_send, stat_recv,
):
    depth, width, height = sizes
    inner = pl.ds(PAD, width)
    places = {axis: lax.axis_index(axis) for axis in ("lat", "lon", "lev")}
    counts = {axis: lax.axis_size(axis) for axis in ("lat", "lon", "lev")}

    def beside(axis, offset):
        return {axis: lax.rem(places[axis] + offset + counts[axis], counts[axis])}

    def rows_of(c):
        return pl.ds(c * rows, rows)

    def load(c):
        return [
            pltpu.make_async_copy(source.at[rows_of(c)], target.at[rows_of(c)], sem.at[c])
            for source, target, sem in (
                (heat_in, raw, load_heat), (ratio_in, ratio, load_ratio), (forcing_in, forcing, load_forcing),
            )
        ]

    def zcopy(side, p, c):
        span = pl.ds(1 + c * rows, rows)
        return pltpu.make_async_remote_copy(
            src_ref=field.at[p, (1, height)[side], span, inner],
            dst_ref=field.at[p, (height + 1, 0)[side], span, inner],
            send_sem=zsend_sem.at[side, p, c], recv_sem=zrecv_sem.at[1 - side, p, c],
            device_id=beside("lev", (-1, 1)[side]), device_id_type=MESH,
        )

    def xcopy(side, p, c):
        return pltpu.make_async_remote_copy(
            src_ref=xsend.at[side, p, c], dst_ref=xrecv.at[1 - side, p, c],
            send_sem=xsend_sem.at[side, p, c], recv_sem=xrecv_sem.at[1 - side, p, c],
            device_id=beside("lon", (-1, 1)[side]), device_id_type=MESH,
        )

    def ycopy(side, p):
        return pltpu.make_async_remote_copy(
            src_ref=field.at[p, pl.ds(1, height), (1, depth)[side], inner],
            dst_ref=field.at[p, pl.ds(1, height), (depth + 1, 0)[side], inner],
            send_sem=ysend_sem.at[side, p], recv_sem=yrecv_sem.at[1 - side, p],
            device_id=beside("lat", (-1, 1)[side]), device_id_type=MESH,
        )

    def stat_copy(offset, c):
        return pltpu.make_async_remote_copy(
            src_ref=stats.at[0, c], dst_ref=stats.at[offset, c],
            send_sem=stat_send.at[offset - 1, c], recv_sem=stat_recv.at[offset - 1, c],
            device_id=beside("lon", offset), device_id_type=MESH,
        )

    def send(p, c):
        for side, end in ((0, 0), (1, chunks - 1)):
            @pl.when(c == end)
            def _():
                ycopy(side, p).start()
        for side in (0, 1):
            zcopy(side, p, c).start()
        for side in (0, 1):
            xcopy(side, p, c).start()

    def sent(p, c):
        for side, end in ((0, 0), (1, chunks - 1)):
            @pl.when(c == end)
            def _():
                ycopy(side, p).wait_send()
        for side in (0, 1):
            zcopy(side, p, c).wait_send()
            xcopy(side, p, c).wait_send()

    def arrived(p, c):
        for side, end in ((1, 0), (0, chunks - 1)):
            @pl.when(c == end)
            def _():
                ycopy(side, p).wait_recv()
        for side in (0, 1):
            xcopy(side, p, c).wait_recv()
        for side in (0, 1):
            zcopy(side, p, c).wait_recv()

    def pack(p, c, i):
        for z in range(height):
            for side, x in ((0, PAD), (1, PAD + width - 1)):
                xsend[side, p, c, pl.ds(i * height + z, 1), :] = field[p, z + 1, c * rows + i + 1, pl.ds(x, 1), :]

    def start_loads(c, carry):
        load(c)[0].start()
        return carry

    def start_others(c, carry):
        for copy in load(c)[1:]:
            copy.start()
        return carry

    barrier = pltpu.get_barrier_semaphore()
    greeted = [beside("lev", -1), beside("lev", 1), beside("lat", -1), beside("lat", 1)]
    greeted += [beside("lon", offset) for offset in range(1, counts["lon"])]
    for device in greeted:
        pl.semaphore_signal(barrier, inc=1, device_id=device, device_id_type=MESH)
    lax.fori_loop(0, chunks, start_loads, 0)

    def unpack(c):
        load(c)[0].wait()

        def row(i, carry):
            y = c * rows + i
            for z in range(height):
                field[0, z + 1, y + 1, inner, :] = raw[y, pl.ds(z, width, stride=height), :]
            pack(0, c, i)
            return carry

        lax.fori_loop(0, rows, row, 0)

    def unpack_send(c, carry):
        unpack(c)
        send(0, c)
        return carry

    unpack(0)
    pl.semaphore_wait(barrier, len(greeted))
    send(0, 0)
    lax.fori_loop(0, chunks, start_others, 0)
    lax.fori_loop(1, chunks, unpack_send, 0)

    def combine(c):
        for offset in range(1, counts["lon"]):
            stat_copy(offset, c).wait_recv()
        means = [stats[offset, c, 0] for offset in range(counts["lon"])]
        mean = sum(means[1:], means[0]) * (1.0 / counts["lon"])
        squares = sum([stats[offset, c, 1] for offset in range(1, counts["lon"])], stats[0, c, 1])
        apart = sum([(other - mean) * (other - mean) for other in means[1:]], (means[0] - mean) * (means[0] - mean))
        variance = (squares + width * apart) * (1.0 / (width * counts["lon"]))
        scale = lax.rsqrt(variance + 0.0001)
        for i in range(rows):
            for half in range(2):
                for kind, values in ((0, mean), (1, scale)):
                    moments_out[kind, c * rows + i, pl.ds(half * height, height), :] = values[i * height:(i + 1) * height]
        for offset in range(1, counts["lon"]):
            stat_copy(offset, c).wait_send()
        sent((STEPS - 1) % 2, c)

    def step(s, carry):
        p = lax.rem(s, 2)
        q = 1 - p

        def chunk(c, carry):
            @pl.when(s == 0)
            def _():
                for copy in load(c)[1:]:
                    copy.wait()

            @pl.when(s >= 1)
            def _():
                sent(q, c)

            arrived(p, c)

            def row(i, carry):
                y = c * rows + i
                for z in range(height):
                    for side, x in ((0, PAD - 1), (1, PAD + width)):
                        field[p, z + 1, y + 1, pl.ds(x, 1), :] = xrecv[side, p, c, pl.ds(i * height + z, 1), :]
                for x in range(0, width, XBLOCK):
                    here = pl.ds(PAD + x, XBLOCK)
                    planes = [field[p, z, y + 1, here, :] for z in range(height + 2)]
                    for z in range(height):
                        middle = planes[z + 1]
                        spread = (
                            field[p, z + 1, y, here, :] + field[p, z + 1, y + 2, here, :]
                            + field[p, z + 1, y + 1, pl.ds(PAD + x - 1, XBLOCK), :]
                            + field[p, z + 1, y + 1, pl.ds(PAD + x + 1, XBLOCK), :]
                            + planes[z] + planes[z + 2] - 6.0 * middle
                        )
                        cells = pl.ds(x * height + z, XBLOCK, stride=height)
                        field[q, z + 1, y + 1, here, :] = middle + ratio[y, cells, :] * spread + forcing[y, cells, :]
                pack(q, c, i)
                return carry

            lax.fori_loop(0, rows, row, 0)

            @pl.when(s < STEPS - 1)
            def _():
                send(q, c)

            @pl.when(s == STEPS - 1)
            def _():
                def finish(i, carry):
                    y = c * rows + i
                    for z in range(height):
                        line = field[q, z + 1, y + 1, inner, :]
                        raw[y, pl.ds(z, width, stride=height), :] = line
                        mean = jnp.sum(line, axis=0, keepdims=True) * (1.0 / width)
                        centred = line - mean
                        stats[0, c, 0, pl.ds(i * height + z, 1), :] = mean
                        stats[0, c, 1, pl.ds(i * height + z, 1), :] = jnp.sum(centred * centred, axis=0, keepdims=True)
                    return carry

                lax.fori_loop(0, rows, finish, 0)
                for offset in range(1, counts["lon"]):
                    stat_copy(offset, c).start()

                @pl.when(c >= 1)
                def _():
                    combine(c - 1)

            return carry

        lax.fori_loop(0, chunks, chunk, 0)
        return carry

    lax.fori_loop(0, STEPS, step, 0)


    combine(chunks - 1)


def score_kernel(chunks, heat, moments, score, end, scaled, score_sem, end_sem):
    rows = heat.shape[0] // chunks
    finish = pltpu.make_async_copy(heat, end, end_sem)
    finish.start()

    def out_copy(c):
        span = pl.ds(c * rows, rows)
        return pltpu.make_async_copy(scaled.at[span], score.at[span], score_sem.at[c])

    def chunk(c, carry):
        def row(i, carry):
            y = c * rows + i
            mean, scale = moments[0, y], moments[1, y]
            values = heat[y]
            tall = values.reshape(values.shape[0] // mean.shape[0], *mean.shape)
            scaled[y] = ((tall - mean[None]) * scale[None]).reshape(values.shape)
            return carry

        lax.fori_loop(0, rows, row, 0)
        out_copy(c).start()
        return carry

    def drain(c, carry):
        out_copy(c).wait()
        return carry

    lax.fori_loop(0, chunks, chunk, 0)
    lax.fori_loop(0, chunks, drain, 0)
    finish.wait()


def local(initial_heat, diffusivity_ratio, forcing_term):
    depth, width, height, members = initial_heat.shape
    rows = 2
    chunks = depth // rows
    lon = lax.axis_size("lon")
    flat = (depth, width * height, members)
    f32 = jnp.float32
    anywhere = pl.BlockSpec(memory_space=pl.ANY)
    dma = pltpu.SemaphoreType.DMA
    heat, moments = pl.pallas_call(
        functools.partial(march_kernel, (depth, width, height), chunks, rows),
        out_shape=(pltpu.VMEM(flat, f32), pltpu.VMEM((2, depth, 2 * height, members), f32)),
        in_specs=[anywhere] * 3,
        out_specs=(pl.BlockSpec(memory_space=pltpu.VMEM),) * 2,
        scratch_shapes=[
            pltpu.VMEM((2, height + 2, depth + 2, width + 2 * PAD, members), f32),
            pltpu.VMEM(flat, f32),
            pltpu.VMEM(flat, f32),
            pltpu.VMEM((2, 2, chunks, rows * height, members), f32),
            pltpu.VMEM((2, 2, chunks, rows * height, members), f32),
            pltpu.VMEM((lon, chunks, 2, rows * height, members), f32),
            dma((chunks,)), dma((chunks,)), dma((chunks,)),
            dma((2, 2, chunks)), dma((2, 2, chunks)),
            dma((2, 2, chunks)), dma((2, 2, chunks)),
            dma((2, 2)), dma((2, 2)),
            dma((lon - 1, chunks)), dma((lon - 1, chunks)),
        ],
        compiler_params=pltpu.CompilerParams(
            collective_id=0, has_side_effects=True, vmem_limit_bytes=48 * 1024 * 1024
        ),
        name="march",
    )(*[a.reshape(flat) for a in (initial_heat, diffusivity_ratio, forcing_term)])
    parts = min(8, depth)
    score, end = pl.pallas_call(
        functools.partial(score_kernel, parts),
        out_shape=(jax.ShapeDtypeStruct(flat, f32),) * 2,
        in_specs=[pl.BlockSpec(memory_space=pltpu.VMEM)] * 2,
        out_specs=(anywhere,) * 2,
        scratch_shapes=[pltpu.VMEM(flat, f32), dma((parts,)), dma(())],
        compiler_params=pltpu.CompilerParams(vmem_limit_bytes=24 * 1024 * 1024),
        name="score",
    )(heat, moments)
    return score.reshape(initial_heat.shape), end.reshape(initial_heat.shape)


def solution(mesh):
    placed = P("lat", "lon", "lev", None)
    return jax.shard_map(
        local, mesh=mesh, in_specs=(placed,) * 3, out_specs=(placed,) * 2, check_vma=False
    )
```
